256 devices in a mesh: dp: 8 (over x, core), cls: 32 (over z, y).
Axes of the slice: x: 4, y: 4, z: 8, core: 2. Of those that a mesh axis runs over, the one named last changes fastest.
Arguments:
- centers: float32 [65536, 512], P('cls'), may hold values from -6 to 6
- momentum: float32 [65536, 512], P('cls'), may hold values from -6 to 6
- grad_rows: bfloat16 [1048576, 512], P(('dp', 'cls')), may hold values from -5400 to 5400
- row_ids: int32 [1048576], P(('dp', 'cls')), may hold values from -1 to 65535, as said below
Outputs:
- new_centers: float32 [65536, 512], P('cls')
- new_momentum: float32 [65536, 512], P('cls')
The draws below stay inside these ranges and needn't reach their ends.
Inputs may be any that keep to these rules, and one draw needn't show every extreme that they name: `row_ids`: slots of one device come in 32 blocks of 128; block o holds only rows o * 2048 to (o + 1) * 2048 - 1 or -1; within a block the used slots come first, distinct and ascending, and one to 128 of them are used. In every draw, for some owner o, every device of some index of dp fills its whole block o.
All inputs are finite; a program needn't handle non-finite values.
Results may differ from the reference program's by a relative error of at most 0.0003.
Values may be sent and summed in bfloat16 or wider, within the bound.
A program may use at most 128 MiB of HBM per device.

```python
import math
import jax
import jax.numpy as jnp
from jax import lax

D = 512
ROWS_DEV = 2048
SAMP_DEV = 4096
CLASSES = 65536
N_DP = 8
N_CLS = 32


def draw_row_ids(key, part):
    capacity = SAMP_DEV // N_CLS
    subkeys = jax.random.split(jax.random.fold_in(key, 11), 3)
    counts = jax.random.randint(subkeys[0], (N_DP, N_CLS, N_CLS), max(capacity // 3, 1), capacity + 1)
    full_owner = jax.random.randint(subkeys[1], (N_DP,), 0, N_CLS)
    owner_line = jnp.arange(N_CLS, dtype=jnp.int32)
    counts = jnp.where(owner_line[None, None, :] == full_owner[:, None, None], capacity, counts)
    scores = jax.random.randint(subkeys[2], (N_DP, N_CLS, N_CLS, ROWS_DEV), 0, 2 ** 30 // ROWS_DEV)
    scores = scores * ROWS_DEV + jnp.arange(ROWS_DEV, dtype=jnp.int32)
    unused, picked = lax.top_k(scores, capacity)
    living = jnp.arange(capacity, dtype=jnp.int32)[None, None, None, :] < counts[..., None]
    ordered_key = jnp.sort(jnp.where(living, picked, ROWS_DEV), axis=-1)
    owner_rows = owner_line[None, None, :, None] * ROWS_DEV
    result = jnp.where(ordered_key < ROWS_DEV, ordered_key + owner_rows, -1)
    return result.reshape(-1).astype(jnp.int32)


def draw_grad_rows(key, part):
    capacity = SAMP_DEV // N_CLS
    subkeys = jax.random.split(jax.random.fold_in(key, 23), 3)
    shape = (N_DP, N_CLS, N_CLS, capacity, D)
    base = jnp.clip(jax.random.normal(subkeys[0], shape, jnp.float32), -6.0, 6.0)
    row_scale = jnp.exp(jax.random.uniform(subkeys[1], (N_DP, N_CLS, N_CLS, capacity, 1), jnp.float32, 0.0, math.log(10.0)))
    col_scale = jnp.exp(jax.random.uniform(subkeys[2], (D,), jnp.float32, 0.0, math.log(10.0)))
    owner_ramp = 3.0 ** (jnp.arange(N_CLS, dtype=jnp.float32) / (N_CLS - 1))
    replica_ramp = 3.0 ** (jnp.arange(N_DP, dtype=jnp.float32) / max(N_DP - 1, 1))
    ramps = replica_ramp[:, None, None, None, None] * owner_ramp[None, None, :, None, None]
    values = base * row_scale * col_scale * ramps
    return values.reshape(N_DP * N_CLS * SAMP_DEV, D).astype(jnp.bfloat16)


def level_of(stream_key, extent, shards, least, high):
    level, own = 1.0, jax.random.fold_in(stream_key, 6)
    for axis_at, shards_of in shards:
        heights = jnp.exp(jax.random.uniform(jax.random.fold_in(own, axis_at), (shards_of,), jnp.float32, least / len(shards), high / len(shards)))
        level = level * jnp.repeat(heights, extent[axis_at] // shards_of).reshape([-1 if axis == axis_at else 1 for axis in range(len(extent))])
    return level


def normal_values(own_key, dims, spread, most, cuts=(), held_as=jnp.bfloat16):
    array = jax.random.normal(own_key, dims, jnp.float32) * spread
    if len(cuts) > 0:
        array = level_of(own_key, dims, cuts, -0.22, 0.18) * array
    return jnp.clip(array, min=-most, max=most).astype(held_as)


def setup_inputs(seed: int = 0) -> dict:
    splits = jax.random.split(jax.random.key(seed), 5)
    centers = normal_values(splits[0], (CLASSES, D), 1.0, 6.0, ((0, 32),), jnp.float32)
    momentum = normal_values(splits[1], (CLASSES, D), 1.0, 6.0, ((0, 32),), jnp.float32)
    grad_rows = draw_grad_rows(jax.random.fold_in(splits[4], 71), 0)
    row_ids = draw_row_ids(jax.random.fold_in(splits[4], 71), 0)
    return dict(centers=centers, momentum=momentum, grad_rows=grad_rows, row_ids=row_ids)


beta_decay = 0.9
learn_rate = 0.5
clip_rms = 1.0
eps_norm = 1e-06
eps_row = 1e-06

def reference(centers, momentum, grad_rows, row_ids):
    targets = jnp.where(row_ids >= 0, row_ids, CLASSES).astype(jnp.int32)
    gradient = jnp.zeros((CLASSES, D), jnp.float32).at[targets].add(grad_rows.astype(jnp.float32), mode='drop')
    squares = jnp.sum(gradient * gradient)
    ceiling = clip_rms * math.sqrt(CLASSES * D)
    factor = jnp.minimum(1.0, ceiling / jnp.sqrt(squares + eps_norm))
    new_momentum = beta_decay * momentum + factor * gradient
    stepped = centers - learn_rate * new_momentum
    rescale = lax.rsqrt(lax.optimization_barrier(jnp.mean(stepped * stepped, axis=1, keepdims=True)) + eps_row)
    return (stepped * rescale, new_momentum)
```

```python
import functools, math
import jax
import jax.numpy as jnp
from jax import lax
from jax.experimental import pallas as pl
from jax.experimental.pallas import tpu as pltpu
from jax.sharding import PartitionSpec as P

MESH = pl.DeviceIdType.MESH
NX, NY, NZ = 4, 4, 8
CAP, WIDE = 128, 128
ROWS = 2048
NCH = 4
CH = ROWS // NCH
HALF = CH // 2
OFFS = (0, 16, 48, 80, 112)
COUNT = (16, 32, 32, 32, 16)
beta_decay, learn_rate, clip_rms, eps_norm, eps_row = 0.9, 0.5, 1.0, 1e-06, 1e-06


def wrap(a, n):
    return lax.rem(a + n, n)


def kernel(rows, ids, g_out, sq_out, raw, idr, zs, zr, fp, dsw, sq1, sq2,
           raw_send, raw_recv, id_send, id_recv, z_send, z_recv, d_send, d_recv,
           a_send, a_recv, f_send, f_recv, s1_send, s1_recv, s2_send, s2_recv):
    d, g = lax.axis_index("dp"), lax.axis_index("cls")
    x, c = lax.div(d, 2), lax.rem(d, 2)
    z, y = lax.div(g, NY), lax.rem(g, NY)
    sgn = 1 - 2 * c
    other = 1 - c

    def dev(xx, cc, yy, zz):
        return (xx * 2 + cc, zz * NY + yy)

    bar = pltpu.get_barrier_semaphore()

    def greet_plane(j, _):
        cc, xx, yy = lax.rem(j, 2), lax.div(j, 8), lax.rem(lax.div(j, 2), NY)
        @pl.when(jnp.logical_or(jnp.logical_or(cc != c, xx != x), yy != y))
        def _():
            pl.semaphore_signal(bar, 1, device_id=dev(xx, cc, yy, z), device_id_type=MESH)
        return 0
    lax.fori_loop(0, 32, greet_plane, 0)

    def greet_z(j, _):
        pl.semaphore_signal(bar, 1, device_id=dev(x, c, y, wrap(z + j, NZ)), device_id_type=MESH)
        return 0
    lax.fori_loop(1, NZ, greet_z, 0)
    pl.semaphore_wait(bar, 31 + NZ - 1)

    me32 = (x * 2 + c) * NY + y

    def id_to(j, _):
        cc, xx, yy = lax.rem(j, 2), lax.div(j, 8), lax.rem(lax.div(j, 2), NY)
        @pl.when(jnp.logical_or(jnp.logical_or(cc != c, xx != x), yy != y))
        def _():
            pltpu.make_async_remote_copy(
                ids.at[:, yy], idr.at[me32], id_send, id_recv,
                device_id=dev(xx, cc, yy, z), device_id_type=MESH).start()
        return 0
    lax.fori_loop(0, 32, id_to, 0)
    pltpu.make_async_copy(ids.at[:, y], idr.at[me32], id_recv).start()

    def send_piece(p):
        k = 4 - p
        slot = OFFS[p] + (me32 if COUNT[p] == 32 else x * NY + y)

        def to(j, cc, zz):
            xx = lax.rem(x + lax.div(j, NY), NX)
            yy = lax.rem(y + lax.rem(j, NY), NY)
            src = rows.at[zz * NY + yy, :, pl.ds(pl.multiple_of(xx * WIDE, WIDE), WIDE)]
            return src, raw.at[slot], dev(xx, cc, yy, z)

        def remote(j, cc, zz):
            src, dst, who = to(j, cc, zz)
            pltpu.make_async_remote_copy(src, dst, raw_send.at[p], raw_recv.at[p],
                                         device_id=who, device_id_type=MESH).start()

        def mine(zz):
            src, dst, _ = to(0, c, zz)
            pltpu.make_async_copy(src, dst, raw_recv.at[p]).start()

        if COUNT[p] == 32:
            def body(j, _):
                remote(j, c, wrap(z + sgn * k, NZ))
                remote(j, other, wrap(z - sgn * k, NZ))
                return 0
            lax.fori_loop(1, NX * NY, body, 0)
            remote(0, other, wrap(z - sgn * k, NZ))
            mine(wrap(z + sgn * k, NZ))
        else:
            def body(j, _):
                remote(j, c, wrap(z + k, NZ))
                return 0
            lax.fori_loop(1, NX * NY, body, 0)
            mine(wrap(z + k, NZ))

    def all_in(ref, sem):
        pltpu.make_async_copy(ref, ref, sem).wait()

    def piece_in(p):
        all_in(raw.at[pl.ds(OFFS[p], COUNT[p])], raw_recv.at[p])

    def piece_out(p):
        all_in(raw.at[pl.ds(0, COUNT[p] - 1)], raw_send.at[p])

    def partial(p, r, out):
        k = 4 - p
        zz = wrap(z + sgn * k, NZ)
        base = (zz * NY + y) * ROWS + r * CH
        line = lax.broadcasted_iota(jnp.int32, (CH, 4 * CAP), 0) + base
        out[...] = jnp.zeros_like(out)

        def step(j, _):
            first = 4 * j if COUNT[p] == 32 else (2 * j + c) * NY
            who = jnp.concatenate([idr[first + t, zz] for t in range(4)], axis=1)
            hot = jnp.where(line == who, 1.0, 0.0).astype(jnp.bfloat16)
            lines = raw[pl.ds(OFFS[p] + 4 * j, 4)].reshape(4 * CAP, WIDE)
            out[...] += jnp.dot(hot, lines, preferred_element_type=jnp.float32)
            return 0
        lax.fori_loop(0, COUNT[p] // 4, step, 0)

    up = wrap(z + sgn, NZ)

    def z_copy(p, r):
        return pltpu.make_async_remote_copy(
            zs.at[p, r], zr.at[p, r], z_send.at[p, r], z_recv.at[p, r],
            device_id=dev(x, c, y, up), device_id_type=MESH)

    for p in range(2):
        send_piece(p)
    all_in(idr, id_recv)
    for p in range(4):
        if p + 2 < 5:
            send_piece(p + 2)
        piece_in(p)
        def chunk(r, _):
            partial(p, r, zs.at[p, r])
            if p:
                z_copy(p - 1, r).wait_recv()
                zs[p, r] = zs[p, r] + zr[p - 1, r]
            z_copy(p, r).start()
            return 0
        lax.fori_loop(0, NCH, chunk, 0)
    piece_in(4)

    mine_x = pl.ds(pl.multiple_of(x * WIDE, WIDE), WIDE)
    def last(r, _):
        partial(4, r, fp.at[r])
        return 0
    lax.fori_loop(0, NCH, last, 0)

    def d_copy(r):
        return pltpu.make_async_remote_copy(
            fp.at[r, pl.ds(pl.multiple_of(other * HALF, HALF), HALF)], dsw.at[r], d_send.at[r], d_recv.at[r],
            device_id=dev(x, other, y, z), device_id_type=MESH)

    def lines_of(r, cc):
        return pl.multiple_of(r * CH + cc * HALF, HALF)

    def a_copy(r, way, xx_slab, part, slot, step):
        to_x = wrap(x + 1 - 2 * way, NX)
        size = HALF // 2 if step else HALF
        at = lines_of(r, c) + (part * size if step else 0)
        ref = g_out.at[pl.ds(pl.multiple_of(at, size), size), pl.ds(pl.multiple_of(xx_slab * WIDE, WIDE), WIDE)]
        return pltpu.make_async_remote_copy(
            ref, ref, a_send.at[r, slot], a_recv.at[r, slot],
            device_id=dev(to_x, c, y, z), device_id_type=MESH)

    def f_copy(r, cc, slab, part, slot):
        size = HALF if part is None else HALF // 2
        at = lines_of(r, cc) + (0 if part is None else part * size)
        ref = g_out.at[pl.ds(pl.multiple_of(at, size), size), pl.ds(pl.multiple_of(slab * WIDE, WIDE), WIDE)]
        return pltpu.make_async_remote_copy(
            ref, ref, f_send.at[r, slot], f_recv.at[r, slot],
            device_id=dev(x, other, y, z), device_id_type=MESH)

    right, left, far = wrap(x + 1, NX), wrap(x - 1, NX), wrap(x + 2, NX)
    total = jnp.zeros((8, 128), jnp.float32)
    for t in range(NCH + 3):
        if t < NCH:
            r = t
            z_copy(3, r).wait_recv()
            fp[r] = fp[r] + zr[3, r]
            d_copy(r).start()
        if 0 <= t - 1 < NCH:
            r = t - 1
            d_copy(r).wait_recv()
            own = fp[r, pl.ds(pl.multiple_of(c * HALF, HALF), HALF)] + dsw[r]
            g_out[pl.ds(lines_of(r, c), HALF), mine_x] = own
            a_copy(r, 0, x, 0, 0, 0).start()
            a_copy(r, 1, x, 0, 1, 0).start()
            f_copy(r, c, x, None, 0).start()
            total = total + jnp.sum((own * own).reshape(HALF // 8, 8, 128), axis=0)
        if t == NCH:
            sq1[me32] = total

            def sq_to(j, _):
                cc, xx, yy = lax.rem(j, 2), lax.div(j, 8), lax.rem(lax.div(j, 2), NY)
                @pl.when(jnp.logical_or(jnp.logical_or(cc != c, xx != x), yy != y))
                def _():
                    pltpu.make_async_remote_copy(
                        sq1.at[me32], sq1.at[me32], s1_send, s1_recv,
                        device_id=dev(xx, cc, yy, z), device_id_type=MESH).start()
                return 0
            lax.fori_loop(0, 32, sq_to, 0)
        if 0 <= t - 2 < NCH:
            r = t - 2
            a_copy(r, 0, left, 0, 0, 0).wait_recv()
            f_copy(r, c, left, None, 1).start()
            a_copy(r, 0, left, 0, 2, 1).start()
            a_copy(r, 1, right, 0, 1, 0).wait_recv()
            f_copy(r, c, right, None, 2).start()
            a_copy(r, 1, right, 1, 3, 1).start()
        if 0 <= t - 3 < NCH:
            r = t - 3
            a_copy(r, 0, far, 0, 2, 1).wait_recv()
            f_copy(r, c, far, 0, 3).start()
            a_copy(r, 1, far, 1, 3, 1).wait_recv()
            f_copy(r, c, far, 1, 4).start()
        if t == NCH + 1:
            all_in(sq1.at[pl.ds(0, 31)], s1_recv)
            sq2[z] = jnp.sum(sq1[...], axis=0)

            def sq_up(j, _):
                pltpu.make_async_remote_copy(
                    sq2.at[z], sq2.at[z], s2_send, s2_recv,
                    device_id=dev(x, c, y, wrap(z + j, NZ)), device_id_type=MESH).start()
                return 0
            lax.fori_loop(1, NZ, sq_up, 0)
    all_in(sq2.at[pl.ds(0, NZ - 1)], s2_recv)
    sq_out[...] = jnp.sum(sq2[...], axis=0)
    for r in range(NCH):
        f_copy(r, other, x, None, 0).wait_recv()
        f_copy(r, other, left, None, 1).wait_recv()
        f_copy(r, other, right, None, 2).wait_recv()
        f_copy(r, other, far, 0, 3).wait_recv()
        f_copy(r, other, far, 1, 4).wait_recv()
    for r in range(NCH):
        d_copy(r).wait_send()
        for slot, step in ((0, 0), (1, 0), (2, 1), (3, 1)):
            a_copy(r, 0, x, 0, slot, step).wait_send()
        for slot, part in ((0, None), (1, None), (2, None), (3, 0), (4, 1)):
            f_copy(r, c, x, part, slot).wait_send()
    all_in(sq1.at[pl.ds(0, 31)], s1_send)
    all_in(sq2.at[pl.ds(0, NZ - 1)], s2_send)
    for p in range(5):
        piece_out(p)
    all_in(idr.at[pl.ds(0, 31)], id_send)
    def done(i, _):
        z_copy(lax.div(i, NCH), lax.rem(i, NCH)).wait_send()
        return 0
    lax.fori_loop(0, 4 * NCH, done, 0)


def exchange(rows, ids):
    dma = pltpu.SemaphoreType.DMA
    f32 = jnp.float32
    return pl.pallas_call(
        kernel,
        out_shape=(jax.ShapeDtypeStruct((ROWS, 512), f32), jax.ShapeDtypeStruct((8, 128), f32)),
        in_specs=[pl.BlockSpec(memory_space=pl.ANY), pl.BlockSpec(memory_space=pltpu.VMEM)],
        out_specs=(pl.BlockSpec(memory_space=pltpu.VMEM), pl.BlockSpec(memory_space=pltpu.VMEM)),
        scratch_shapes=[
            pltpu.VMEM((128, CAP, WIDE), jnp.bfloat16),
            pltpu.VMEM((32, NZ, 1, CAP), jnp.int32),
            pltpu.VMEM((4, NCH, CH, WIDE), f32),
            pltpu.VMEM((4, NCH, CH, WIDE), f32),
            pltpu.VMEM((NCH, CH, WIDE), f32),
            pltpu.VMEM((NCH, HALF, WIDE), f32),
            pltpu.VMEM((32, 8, 128), f32),
            pltpu.VMEM((NZ, 8, 128), f32),
            dma((5,)), dma((5,)), dma, dma,
            dma((4, NCH)), dma((4, NCH)), dma((NCH,)), dma((NCH,)),
            dma((NCH, 4)), dma((NCH, 4)), dma((NCH, 5)), dma((NCH, 5)),
            dma, dma, dma, dma,
        ],
        compiler_params=pltpu.CompilerParams(collective_id=0, has_side_effects=True,
                                             vmem_limit_bytes=50 * 2 ** 20),
        name="exchange",
    )(rows, ids)


def update_kernel(sq, g, m, cen, new_c, new_m):
    squares = jnp.sum(sq[...], keepdims=True)
    factor = jnp.minimum(1.0, clip_rms * math.sqrt(65536 * 512) / jnp.sqrt(squares + eps_norm))
    mom = beta_decay * m[...] + factor * g[...]
    new_m[...] = mom
    stepped = cen[...] - learn_rate * mom
    rescale = lax.rsqrt(jnp.mean(stepped * stepped, axis=1, keepdims=True) + eps_row)
    new_c[...] = stepped * rescale


def update(sq, g, m, cen):
    tile = 256
    spec = pl.BlockSpec((tile, 512), lambda i: (i, 0))
    shape = jax.ShapeDtypeStruct((ROWS, 512), jnp.float32)
    return pl.pallas_call(
        update_kernel,
        grid=(ROWS // tile,),
        out_shape=(shape, shape),
        in_specs=[pl.BlockSpec((8, 128), lambda i: (0, 0)), spec, spec, spec],
        out_specs=(spec, spec),
        name="update",
    )(sq, g, m, cen)


def on_device(centers, momentum, grad_rows, row_ids):
    g, sq = exchange(grad_rows.reshape(32, CAP, 512), row_ids.reshape(NZ, NY, 1, CAP))
    return update(sq, g, momentum, centers)


def solution(mesh):
    placed = (P("cls", None), P("cls", None), P(("dp", "cls"), None), P(("dp", "cls")))
    return jax.shard_map(
        on_device,
        mesh=mesh,
        in_specs=placed,
        out_specs=(P("cls", None), P("cls", None)),
        check_vma=False,
    )
```

```python
import functools, math
import jax
import jax.numpy as jnp
from jax import lax
from jax.experimental import pallas as pl
from jax.experimental.pallas import tpu as pltpu
from jax.sharding import PartitionSpec as P

MESH = pl.DeviceIdType.MESH
BF = jnp.bfloat16
NX, NY, NZ = 4, 4, 8
CAP, WIDE = 128, 128
ROWS = 2048
UNIT = NX * NY
HIGH = 4
LOW = ROWS // HIGH
NCH = 8
CH = ROWS // NCH
HALF = CH // 2
LAG_A, LAG_F, LAG_S = 3, 5, 3
TILE = 256
RING = 4
COUNT = (16, 32, 32, 32, 16)
UNITS = ((0,), (1, 2), (3, 4), (5, 6), (7,))
PIECE = (0, 1, 1, 2, 2, 3, 3, 4)
beta_decay, learn_rate, clip_rms, eps_norm, eps_row = 0.9, 0.5, 1.0, 1e-06, 1e-06


def wrap(a, n):
    return lax.rem(a + n, n)


def kernel(rows, ids, mom, cen, g_out, sq_out, mom_out, cen_out, raw, idr, hot, high, wide, zs, zr, fp, dsw, sq1, sq2,
           raw_send, raw_recv, id_send, id_recv, z_send, z_recv, d_send, d_recv,
           a_send, a_recv, f_send, f_recv, s1_send, s1_recv, s2_send, s2_recv, keep):
    d, g = lax.axis_index("dp"), lax.axis_index("cls")
    x, c = lax.div(d, 2), lax.rem(d, 2)
    z, y = lax.div(g, NY), lax.rem(g, NY)
    sgn = 1 - 2 * c
    other = 1 - c

    def dev(xx, cc, yy, zz):
        return (xx * 2 + cc, zz * NY + yy)

    bar = pltpu.get_barrier_semaphore()

    def greet_plane(j, _):
        cc, xx, yy = lax.rem(j, 2), lax.div(j, 8), lax.rem(lax.div(j, 2), NY)
        @pl.when(jnp.logical_or(jnp.logical_or(cc != c, xx != x), yy != y))
        def _():
            pl.semaphore_signal(bar, 1, device_id=dev(xx, cc, yy, z), device_id_type=MESH)
        return 0
    lax.fori_loop(0, 32, greet_plane, 0)

    def greet_z(j, _):
        pl.semaphore_signal(bar, 1, device_id=dev(x, c, y, wrap(z + j, NZ)), device_id_type=MESH)
        return 0
    lax.fori_loop(1, NZ, greet_z, 0)
    pl.semaphore_wait(bar, 31 + NZ - 1)

    me32 = c * UNIT + x * NY + y

    def place(t, dx):
        return t * 2 * NX + dx * 2 + c

    def id_round(t, _):
        for dx in range(NX):
            for cc in range(2):
                xx, yy = lax.rem(x + dx, NX), lax.rem(y + dx + t + c, NY)

                def send():
                    pltpu.make_async_remote_copy(
                        ids.at[:, yy], idr.at[place(t, dx)], id_send, id_recv,
                        device_id=dev(xx, cc, yy, z), device_id_type=MESH).start()
                if dx:
                    send()
                else:
                    pl.when(jnp.logical_or(yy != y, cc != c))(send)
        return 0
    lax.fori_loop(0, NY, id_round, 0)
    home = lax.rem(NY - c, NY)
    pltpu.make_async_copy(ids.at[:, y], idr.at[place(home, 0)], id_recv).start()

    def momentum_in():
        pltpu.make_async_copy(mom, mom_out, keep.at[0]).start()
        pltpu.make_async_copy(cen, cen_out, keep.at[1]).start()

    def send_piece(p):
        k = 4 - p
        full = COUNT[p] == 32
        near, away = wrap(z + (sgn if full else 1) * k, NZ), wrap(z - sgn * k, NZ)

        def where_to(t, dx):
            if full:
                unit = UNITS[p][0] + lax.div(t, 2)
                return unit, UNITS[p][0] * UNIT + place(t, dx)
            return UNITS[p][0], UNITS[p][0] * UNIT + t * NX + dx

        def lines(xx, yy, zz):
            return rows.at[zz * NY + yy, :, pl.ds(pl.multiple_of(xx * WIDE, WIDE), WIDE)]

        def remote(t, dx, xx, yy, cc, zz):
            unit, slot = where_to(t, dx)
            pltpu.make_async_remote_copy(lines(xx, yy, zz), raw.at[slot], raw_send.at[p], raw_recv.at[unit],
                                         device_id=dev(xx, cc, yy, z), device_id_type=MESH).start()

        def round_of(t, _):
            for dx in range(NX):
                xx, yy = lax.rem(x + dx, NX), lax.rem(y + dx + t + c, NY)

                def both():
                    remote(t, dx, xx, yy, c, near)
                    if full:
                        remote(t, dx, xx, yy, other, away)
                if dx:
                    both()
                else:
                    pl.when(yy != y)(both)
            return 0
        lax.fori_loop(0, NY, round_of, 0)
        if full:
            remote(home, 0, x, y, other, away)
        unit, slot = where_to(home, 0)
        pltpu.make_async_copy(lines(x, y, near), raw.at[slot], raw_recv.at[unit]).start()

    def all_in(ref, sem):
        pltpu.make_async_copy(ref, ref, sem).wait()

    def unit_in(u):
        all_in(raw.at[pl.ds(u * UNIT, UNIT)], raw_recv.at[u])

    def piece_out(p):
        all_in(raw.at[pl.ds(0, COUNT[p] - 1)], raw_send.at[p])

    def prepare(u):
        p = PIECE[u]
        zz = wrap(z + sgn * (4 - p), NZ)
        base = (zz * NY + y) * ROWS

        def local(b):
            at = 2 * b + c if COUNT[p] == 16 else (u + 1) % 2 * UNIT + b
            return idr[at, zz] - base

        def block(b, _):
            part = jnp.right_shift(local(b), LOW.bit_length() - 1).astype(jnp.float32)
            high[u % RING * UNIT + b] = jnp.broadcast_to(part, (CAP, WIDE)).T.astype(BF)
            return 0
        lax.fori_loop(0, UNIT, block, 0, unroll=4)
        line = lax.broadcasted_iota(jnp.int32, (LOW, 2 * CAP), 0)
        for q in range(UNIT // 2):
            low = jnp.bitwise_and(jnp.concatenate([local(2 * q), local(2 * q + 1)], axis=1), LOW - 1)
            hot[u % RING, :, q * 2 * CAP:(q + 1) * 2 * CAP] = jnp.where(line == low, 1.0, 0.0).astype(BF)

    def compute(u, out, add):
        for b in range(UNIT):
            lines, part = raw[u * UNIT + b], high[u % RING * UNIT + b]
            for h in range(HIGH):
                wide[b * CAP:(b + 1) * CAP, h * WIDE:(h + 1) * WIDE] = jnp.where(
                    part == jnp.asarray(h, BF), lines, jnp.zeros_like(lines))
        for n in range(HIGH // 2):
            v = jnp.dot(hot[u % RING], wide[:, 2 * n * WIDE:2 * (n + 1) * WIDE], preferred_element_type=jnp.float32)
            for q in range(2):
                at = pl.ds((2 * n + q) * LOW, LOW)
                now = v[:, q * WIDE:(q + 1) * WIDE]
                out[at, :] = out[at, :] + now if add else now

    up = wrap(z + sgn, NZ)

    def rows_at(r):
        return pl.ds(pl.multiple_of(r * CH, CH), CH)

    def z_copy(p, r):
        return pltpu.make_async_remote_copy(
            zs.at[p, rows_at(r)], zr.at[p, rows_at(r)], z_send.at[p, r], z_recv.at[p, r],
            device_id=dev(x, c, y, up), device_id_type=MESH)

    for p in range(2):
        send_piece(p)
    momentum_in()
    all_in(idr, id_recv)
    for u in range(3):
        prepare(u)
    for p in range(4):
        if p + 2 < 5:
            send_piece(p + 2)
        for u in UNITS[p]:
            unit_in(u)
            compute(u, zs.at[p], u != UNITS[p][0])

        def chunk(r, _):
            if p:
                z_copy(p - 1, r).wait_recv()
                zs[p, rows_at(r)] = zs[p, rows_at(r)] + zr[p - 1, rows_at(r)]
            z_copy(p, r).start()
            return 0
        lax.fori_loop(0, NCH, chunk, 0)
        for u in UNITS[p]:
            if u + 3 < 8:
                prepare(u + 3)
    unit_in(7)

    mine_x = pl.ds(pl.multiple_of(x * WIDE, WIDE), WIDE)
    compute(7, fp, False)

    def d_copy(r):
        return pltpu.make_async_remote_copy(
            fp.at[pl.ds(lines_of(r, other), HALF)], dsw.at[r], d_send.at[r], d_recv.at[r],
            device_id=dev(x, other, y, z), device_id_type=MESH)

    def lines_of(r, cc):
        return pl.multiple_of(r * CH + cc * HALF, HALF)

    def a_copy(r, way, xx_slab, part, slot, step):
        to_x = wrap(x + 1 - 2 * way, NX)
        size = HALF // 2 if step else HALF
        at = lines_of(r, c) + (part * size if step else 0)
        ref = g_out.at[pl.ds(pl.multiple_of(at, size), size), pl.ds(pl.multiple_of(xx_slab * WIDE, WIDE), WIDE)]
        return pltpu.make_async_remote_copy(
            ref, ref, a_send.at[r, slot], a_recv.at[r, slot],
            device_id=dev(to_x, c, y, z), device_id_type=MESH)

    def f_copy(r, cc, slab, part, slot):
        size = HALF if part is None else HALF // 2
        at = lines_of(r, cc) + (0 if part is None else part * size)
        ref = g_out.at[pl.ds(pl.multiple_of(at, size), size), pl.ds(pl.multiple_of(slab * WIDE, WIDE), WIDE)]
        return pltpu.make_async_remote_copy(
            ref, ref, f_send.at[r, slot], f_recv.at[r, slot],
            device_id=dev(x, other, y, z), device_id_type=MESH)

    right, left, far = wrap(x + 1, NX), wrap(x - 1, NX), wrap(x + 2, NX)
    total = jnp.zeros((8, 128), jnp.float32)
    for t in range(NCH + LAG_F):
        if t < NCH:
            r = t
            z_copy(3, r).wait_recv()
            fp[rows_at(r)] = fp[rows_at(r)] + zr[3, rows_at(r)]
            d_copy(r).start()
        if 0 <= t - 1 < NCH:
            r = t - 1
            d_copy(r).wait_recv()
            own = fp[pl.ds(lines_of(r, c), HALF)] + dsw[r]
            g_out[pl.ds(lines_of(r, c), HALF), mine_x] = own
            a_copy(r, 0, x, 0, 0, 0).start()
            a_copy(r, 1, x, 0, 1, 0).start()
            f_copy(r, c, x, None, 0).start()
            total = total + jnp.sum((own * own).reshape(HALF // 8, 8, 128), axis=0)
        if t == NCH:
            sq2[z] = total

            def sq_up(j, _):
                pltpu.make_async_remote_copy(
                    sq2.at[z], sq2.at[z], s2_send, s2_recv,
                    device_id=dev(x, c, y, wrap(z + j, NZ)), device_id_type=MESH).start()
                return 0
            lax.fori_loop(1, NZ, sq_up, 0)
        if 0 <= t - LAG_A < NCH:
            r = t - LAG_A
            a_copy(r, 0, left, 0, 0, 0).wait_recv()
            f_copy(r, c, left, None, 1).start()
            a_copy(r, 0, left, 0, 2, 1).start()
            a_copy(r, 1, right, 0, 1, 0).wait_recv()
            f_copy(r, c, right, None, 2).start()
            a_copy(r, 1, right, 1, 3, 1).start()
        if 0 <= t - LAG_F < NCH:
            r = t - LAG_F
            a_copy(r, 0, far, 0, 2, 1).wait_recv()
            f_copy(r, c, far, 0, 3).start()
            a_copy(r, 1, far, 1, 3, 1).wait_recv()
            f_copy(r, c, far, 1, 4).start()
        if t == NCH + LAG_S:
            all_in(sq2.at[pl.ds(0, NZ - 1)], s2_recv)
            sq1[me32] = jnp.sum(sq2[...], axis=0)

            def sq_to(j, _):
                cc, xx, yy = lax.rem(j, 2), lax.div(j, 8), lax.rem(lax.div(j, 2), NY)
                @pl.when(jnp.logical_or(jnp.logical_or(cc != c, xx != x), yy != y))
                def _():
                    pltpu.make_async_remote_copy(
                        sq1.at[me32], sq1.at[me32], s1_send, s1_recv,
                        device_id=dev(xx, cc, yy, z), device_id_type=MESH).start()
                return 0
            lax.fori_loop(0, 32, sq_to, 0)
    for r in range(NCH):
        f_copy(r, other, x, None, 0).wait_recv()
        f_copy(r, other, left, None, 1).wait_recv()
        f_copy(r, other, right, None, 2).wait_recv()
        f_copy(r, other, far, 0, 3).wait_recv()
        f_copy(r, other, far, 1, 4).wait_recv()
    all_in(sq1.at[pl.ds(0, 31)], s1_recv)
    sq_out[...] = jnp.sum(sq1[...], axis=0)
    for r in range(NCH):
        d_copy(r).wait_send()
        for slot, step in ((0, 0), (1, 0), (2, 1), (3, 1)):
            a_copy(r, 0, x, 0, slot, step).wait_send()
        for slot, part in ((0, None), (1, None), (2, None), (3, 0), (4, 1)):
            f_copy(r, c, x, part, slot).wait_send()
    all_in(sq1.at[pl.ds(0, 31)], s1_send)
    all_in(sq2.at[pl.ds(0, NZ - 1)], s2_send)
    pltpu.make_async_copy(mom, mom_out, keep.at[0]).wait()
    pltpu.make_async_copy(cen, cen_out, keep.at[1]).wait()
    for p in range(5):
        piece_out(p)
    all_in(idr.at[pl.ds(0, 31)], id_send)
    def done(i, _):
        z_copy(lax.div(i, NCH), lax.rem(i, NCH)).wait_send()
        return 0
    lax.fori_loop(0, 4 * NCH, done, 0)


def exchange(rows, ids, mom, cen):
    dma = pltpu.SemaphoreType.DMA
    f32 = jnp.float32
    table = jax.ShapeDtypeStruct((ROWS, 512), f32)
    return pl.pallas_call(
        kernel,
        out_shape=(table, jax.ShapeDtypeStruct((8, 128), f32), table, table),
        in_specs=[pl.BlockSpec(memory_space=pltpu.HBM)] * 4,
        out_specs=(pl.BlockSpec(memory_space=pltpu.VMEM),) * 4,
        scratch_shapes=[
            pltpu.VMEM((128, CAP, WIDE), jnp.bfloat16),
            pltpu.VMEM((32, NZ, 1, CAP), jnp.int32),
            pltpu.VMEM((RING, LOW, UNIT * CAP), BF),
            pltpu.VMEM((RING * UNIT, CAP, WIDE), BF),
            pltpu.VMEM((UNIT * CAP, HIGH * WIDE), BF),
            pltpu.VMEM((4, ROWS, WIDE), f32),
            pltpu.VMEM((4, ROWS, WIDE), f32),
            pltpu.VMEM((ROWS, WIDE), f32),
            pltpu.VMEM((NCH, HALF, WIDE), f32),
            pltpu.VMEM((32, 8, 128), f32),
            pltpu.VMEM((NZ, 8, 128), f32),
            dma((5,)), dma((8,)), dma, dma,
            dma((4, NCH)), dma((4, NCH)), dma((NCH,)), dma((NCH,)),
            dma((NCH, 4)), dma((NCH, 4)), dma((NCH, 5)), dma((NCH, 5)),
            dma, dma, dma, dma, dma((2,)),
        ],
        compiler_params=pltpu.CompilerParams(collective_id=0, has_side_effects=True,
                                             vmem_limit_bytes=40 * 2 ** 20),
        name="exchange",
    )(rows, ids, mom, cen)


def update_kernel(sq, g, m, cen, new_c, new_m):
    squares = jnp.sum(sq[...], keepdims=True)
    factor = jnp.minimum(1.0, clip_rms * math.sqrt(65536 * 512) / jnp.sqrt(squares + eps_norm))
    at = pl.ds(pl.multiple_of(pl.program_id(0) * TILE, TILE), TILE)
    mom = beta_decay * m[at] + factor * g[at]
    new_m[...] = mom
    stepped = cen[at] - learn_rate * mom
    rescale = lax.rsqrt(jnp.mean(stepped * stepped, axis=1, keepdims=True) + eps_row)
    new_c[...] = stepped * rescale


def update(sq, g, m, cen):
    spec = pl.BlockSpec((TILE, 512), lambda i: (i, 0))
    shape = jax.ShapeDtypeStruct((ROWS, 512), jnp.float32)
    return pl.pallas_call(
        update_kernel,
        grid=(ROWS // TILE,),
        out_shape=(shape, shape),
        in_specs=[pl.BlockSpec(memory_space=pltpu.VMEM)] * 4,
        out_specs=(spec, spec),
        compiler_params=pltpu.CompilerParams(vmem_limit_bytes=20 * 2 ** 20),
        name="update",
    )(sq, g, m, cen)


def on_device(centers, momentum, grad_rows, row_ids):
    g, sq, mom, cen = exchange(
        grad_rows.reshape(32, CAP, 512), row_ids.reshape(NZ, NY, 1, CAP), momentum, centers)
    return update(sq, g, mom, cen)


def solution(mesh):
    placed = (P("cls", None), P("cls", None), P(("dp", "cls"), None), P(("dp", "cls")))
    return jax.shard_map(
        on_device,
        mesh=mesh,
        in_specs=placed,
        out_specs=(P("cls", None), P("cls", None)),
        check_vma=False,
    )
```

```python
import functools, math
import jax
import jax.numpy as jnp
from jax import lax
from jax.experimental import pallas as pl
from jax.experimental.pallas import tpu as pltpu
from jax.sharding import PartitionSpec as P

MESH = pl.DeviceIdType.MESH
BF = jnp.bfloat16
NX, NY, NZ = 4, 4, 8
CAP, WIDE = 128, 128
ROWS = 2048
UNIT = NX * NY
HIGH = 4
LOW = ROWS // HIGH
NCH = 8
CH = ROWS // NCH
HALF = CH // 2
LAG_D, LAG_A, LAG_F, LAG_S = 2, 5, 9, 2
TILE = 128
RING = 4
COUNT = (16, 32, 32, 32, 16)
UNITS = ((0,), (1, 2), (3, 4), (5, 6), (7,))
PIECE = (0, 1, 1, 2, 2, 3, 3, 4)
beta_decay, learn_rate, clip_rms, eps_norm, eps_row = 0.9, 0.5, 1.0, 1e-06, 1e-06


def wrap(a, n):
    return lax.rem(a + n, n)


def kernel(rows, ids, mom, cen, g_out, sq_out, mom_out, cen_out, raw, idr, hot, high, wide, zs, zr, fp, dsw, sq1, sq2,
           raw_send, raw_recv, id_send, id_recv, z_send, z_recv, d_send, d_recv,
           a_send, a_recv, f_send, f_recv, s1_send, s1_recv, s2_send, s2_recv, keep):
    d, g = lax.axis_index("dp"), lax.axis_index("cls")
    x, c = lax.div(d, 2), lax.rem(d, 2)
    z, y = lax.div(g, NY), lax.rem(g, NY)
    sgn = 1 - 2 * c
    other = 1 - c

    def dev(xx, cc, yy, zz):
        return (xx * 2 + cc, zz * NY + yy)

    bar = pltpu.get_barrier_semaphore()

    def greet_plane(j, _):
        cc, xx, yy = lax.rem(j, 2), lax.div(j, 8), lax.rem(lax.div(j, 2), NY)
        @pl.when(jnp.logical_or(jnp.logical_or(cc != c, xx != x), yy != y))
        def _():
            pl.semaphore_signal(bar, 1, device_id=dev(xx, cc, yy, z), device_id_type=MESH)
        return 0
    lax.fori_loop(0, 32, greet_plane, 0)

    def greet_z(j, _):
        pl.semaphore_signal(bar, 1, device_id=dev(x, c, y, wrap(z + j, NZ)), device_id_type=MESH)
        return 0
    lax.fori_loop(1, NZ, greet_z, 0)
    pl.semaphore_wait(bar, 31 + NZ - 1)

    me32 = c * UNIT + x * NY + y

    def place(t, dx):
        return t * 2 * NX + dx * 2 + c

    def id_round(t, _):
        for dx in range(NX):
            for cc in range(2):
                xx, yy = lax.rem(x + dx, NX), lax.rem(y + dx + t + c, NY)

                def send():
                    pltpu.make_async_remote_copy(
                        ids.at[:, yy], idr.at[place(t, dx)], id_send, id_recv,
                        device_id=dev(xx, cc, yy, z), device_id_type=MESH).start()
                if dx:
                    send()
                else:
                    pl.when(jnp.logical_or(yy != y, cc != c))(send)
        return 0
    lax.fori_loop(0, NY, id_round, 0)
    home = lax.rem(NY - c, NY)
    pltpu.make_async_copy(ids.at[:, y], idr.at[place(home, 0)], id_recv).start()

    def momentum_in():
        pltpu.make_async_copy(mom, mom_out, keep.at[0]).start()
        pltpu.make_async_copy(cen, cen_out, keep.at[1]).start()

    def send_piece(p):
        k = 4 - p
        full = COUNT[p] == 32
        near, away = wrap(z + (sgn if full else 1) * k, NZ), wrap(z - sgn * k, NZ)

        def where_to(t, dx):
            if full:
                unit = UNITS[p][0] + lax.div(t, 2)
                return unit, UNITS[p][0] * UNIT + place(t, dx)
            return UNITS[p][0], UNITS[p][0] * UNIT + t * NX + dx

        def lines(xx, yy, zz):
            return rows.at[zz * NY + yy, :, pl.ds(pl.multiple_of(xx * WIDE, WIDE), WIDE)]

        def remote(t, dx, xx, yy, cc, zz):
            unit, slot = where_to(t, dx)
            pltpu.make_async_remote_copy(lines(xx, yy, zz), raw.at[slot], raw_send.at[p], raw_recv.at[unit],
                                         device_id=dev(xx, cc, yy, z), device_id_type=MESH).start()

        def round_of(t, _):
            for dx in range(NX):
                xx, yy = lax.rem(x + dx, NX), lax.rem(y + dx + t + c, NY)

                def both():
                    remote(t, dx, xx, yy, c, near)
                    if full:
                        remote(t, dx, xx, yy, other, away)
                if dx:
                    both()
                else:
                    pl.when(yy != y)(both)
            return 0
        lax.fori_loop(0, NY, round_of, 0)
        if full:
            remote(home, 0, x, y, other, away)
        unit, slot = where_to(home, 0)
        pltpu.make_async_copy(lines(x, y, near), raw.at[slot], raw_recv.at[unit]).start()

    def all_in(ref, sem):
        pltpu.make_async_copy(ref, ref, sem).wait()

    def unit_in(u):
        all_in(raw.at[pl.ds(u * UNIT, UNIT)], raw_recv.at[u])

    def piece_out(p):
        all_in(raw.at[pl.ds(0, COUNT[p] - 1)], raw_send.at[p])

    def prepare(u):
        p = PIECE[u]
        zz = wrap(z + sgn * (4 - p), NZ)
        base = (zz * NY + y) * ROWS

        def local(b):
            at = 2 * b + c if COUNT[p] == 16 else (u + 1) % 2 * UNIT + b
            return idr[at, zz] - base

        def block(b, _):
            part = jnp.right_shift(local(b), LOW.bit_length() - 1).astype(jnp.float32)
            high[u % RING * UNIT + b] = jnp.broadcast_to(part, (CAP, WIDE)).T.astype(BF)
            return 0
        lax.fori_loop(0, UNIT, block, 0, unroll=4)
        line = lax.broadcasted_iota(jnp.int32, (LOW, 2 * CAP), 0)
        for q in range(UNIT // 2):
            low = jnp.bitwise_and(jnp.concatenate([local(2 * q), local(2 * q + 1)], axis=1), LOW - 1)
            hot[u % RING, :, q * 2 * CAP:(q + 1) * 2 * CAP] = jnp.where(line == low, 1.0, 0.0).astype(BF)

    def compute(u, out, add):
        for b in range(UNIT):
            lines, part = raw[u * UNIT + b], high[u % RING * UNIT + b]
            for h in range(HIGH):
                wide[b * CAP:(b + 1) * CAP, h * WIDE:(h + 1) * WIDE] = jnp.where(
                    part == jnp.asarray(h, BF), lines, jnp.zeros_like(lines))
        for n in range(HIGH // 2):
            v = jnp.dot(hot[u % RING], wide[:, 2 * n * WIDE:2 * (n + 1) * WIDE], preferred_element_type=jnp.float32)
            for q in range(2):
                at = pl.ds((2 * n + q) * LOW, LOW)
                now = v[:, q * WIDE:(q + 1) * WIDE]
                out[at, :] = out[at, :] + now if add else now

    up = wrap(z + sgn, NZ)

    def rows_at(r):
        return pl.ds(pl.multiple_of(r * CH, CH), CH)

    def z_copy(p, r):
        return pltpu.make_async_remote_copy(
            zs.at[p, rows_at(r)], zr.at[p, rows_at(r)], z_send.at[p, r], z_recv.at[p, r],
            device_id=dev(x, c, y, up), device_id_type=MESH)

    for p in range(2):
        send_piece(p)
    momentum_in()
    all_in(idr, id_recv)
    for u in range(3):
        prepare(u)
    for p in range(4):
        if p + 2 < 5:
            send_piece(p + 2)
        for u in UNITS[p]:
            unit_in(u)
            compute(u, zs.at[p], u != UNITS[p][0])

        def chunk(r, _):
            if p:
                z_copy(p - 1, r).wait_recv()
                zs[p, rows_at(r)] = zs[p, rows_at(r)] + zr[p - 1, rows_at(r)]
            z_copy(p, r).start()
            return 0
        lax.fori_loop(0, NCH, chunk, 0)
        for u in UNITS[p]:
            if u + 3 < 8:
                prepare(u + 3)
    unit_in(7)

    mine_x = pl.ds(pl.multiple_of(x * WIDE, WIDE), WIDE)
    compute(7, fp, False)

    def d_copy(r):
        return pltpu.make_async_remote_copy(
            fp.at[pl.ds(lines_of(r, other), HALF)], dsw.at[r], d_send.at[r], d_recv.at[r],
            device_id=dev(x, other, y, z), device_id_type=MESH)

    def lines_of(r, cc):
        return pl.multiple_of(r * CH + cc * HALF, HALF)

    def a_copy(r, way, xx_slab, part, slot, step):
        to_x = wrap(x + 1 - 2 * way, NX)
        size = HALF // 2 if step else HALF
        at = lines_of(r, c) + (part * size if step else 0)
        ref = g_out.at[pl.ds(pl.multiple_of(at, size), size), pl.ds(pl.multiple_of(xx_slab * WIDE, WIDE), WIDE)]
        return pltpu.make_async_remote_copy(
            ref, ref, a_send.at[r, slot], a_recv.at[r, slot],
            device_id=dev(to_x, c, y, z), device_id_type=MESH)

    def f_copy(r, cc, slab, part, slot):
        size = HALF if part is None else HALF // 2
        at = lines_of(r, cc) + (0 if part is None else part * size)
        ref = g_out.at[pl.ds(pl.multiple_of(at, size), size), pl.ds(pl.multiple_of(slab * WIDE, WIDE), WIDE)]
        return pltpu.make_async_remote_copy(
            ref, ref, f_send.at[r, slot], f_recv.at[r, slot],
            device_id=dev(x, other, y, z), device_id_type=MESH)

    right, left, far = wrap(x + 1, NX), wrap(x - 1, NX), wrap(x + 2, NX)
    total = jnp.zeros((8, 128), jnp.float32)
    for t in range(NCH + LAG_F):
        if t < NCH:
            r = t
            z_copy(3, r).wait_recv()
            fp[rows_at(r)] = fp[rows_at(r)] + zr[3, rows_at(r)]
            d_copy(r).start()
        if 0 <= t - LAG_D < NCH:
            r = t - LAG_D
            d_copy(r).wait_recv()
            own = fp[pl.ds(lines_of(r, c), HALF)] + dsw[r]
            g_out[pl.ds(lines_of(r, c), HALF), mine_x] = own
            a_copy(r, 0, x, 0, 0, 0).start()
            a_copy(r, 1, x, 0, 1, 0).start()
            f_copy(r, c, x, None, 0).start()
            total = total + jnp.sum((own * own).reshape(HALF // 8, 8, 128), axis=0)
        if t == NCH - 1 + LAG_D:
            sq2[z] = jnp.sum(total, axis=0, keepdims=True)

            def sq_up(j, _):
                pltpu.make_async_remote_copy(
                    sq2.at[z], sq2.at[z], s2_send, s2_recv,
                    device_id=dev(x, c, y, wrap(z + j, NZ)), device_id_type=MESH).start()
                return 0
            lax.fori_loop(1, NZ, sq_up, 0)
        if 0 <= t - LAG_A < NCH:
            r = t - LAG_A
            a_copy(r, 0, left, 0, 0, 0).wait_recv()
            f_copy(r, c, left, None, 1).start()
            a_copy(r, 0, left, 0, 2, 1).start()
            a_copy(r, 1, right, 0, 1, 0).wait_recv()
            f_copy(r, c, right, None, 2).start()
            a_copy(r, 1, right, 1, 3, 1).start()
        if 0 <= t - LAG_F < NCH:
            r = t - LAG_F
            a_copy(r, 0, far, 0, 2, 1).wait_recv()
            f_copy(r, c, far, 0, 3).start()
            a_copy(r, 1, far, 1, 3, 1).wait_recv()
            f_copy(r, c, far, 1, 4).start()
        if t == NCH - 1 + LAG_D + LAG_S:
            all_in(sq2.at[pl.ds(0, NZ - 1)], s2_recv)
            sq1[me32] = jnp.sum(sq2[...], axis=0)

            def sq_to(j, _):
                cc, xx, yy = lax.rem(j, 2), lax.div(j, 8), lax.rem(lax.div(j, 2), NY)
                @pl.when(jnp.logical_or(jnp.logical_or(cc != c, xx != x), yy != y))
                def _():
                    pltpu.make_async_remote_copy(
                        sq1.at[me32], sq1.at[me32], s1_send, s1_recv,
                        device_id=dev(xx, cc, yy, z), device_id_type=MESH).start()
                return 0
            lax.fori_loop(0, 32, sq_to, 0)
    for r in range(NCH):
        f_copy(r, other, x, None, 0).wait_recv()
        f_copy(r, other, left, None, 1).wait_recv()
        f_copy(r, other, right, None, 2).wait_recv()
        f_copy(r, other, far, 0, 3).wait_recv()
        f_copy(r, other, far, 1, 4).wait_recv()
    all_in(sq1.at[pl.ds(0, 31)], s1_recv)
    sq_out[...] = jnp.sum(sq1[...], axis=0)
    for r in range(NCH):
        d_copy(r).wait_send()
        for slot, step in ((0, 0), (1, 0), (2, 1), (3, 1)):
            a_copy(r, 0, x, 0, slot, step).wait_send()
        for slot, part in ((0, None), (1, None), (2, None), (3, 0), (4, 1)):
            f_copy(r, c, x, part, slot).wait_send()
    all_in(sq1.at[pl.ds(0, 31)], s1_send)
    all_in(sq2.at[pl.ds(0, NZ - 1)], s2_send)
    pltpu.make_async_copy(mom, mom_out, keep.at[0]).wait()
    pltpu.make_async_copy(cen, cen_out, keep.at[1]).wait()
    for p in range(5):
        piece_out(p)
    all_in(idr.at[pl.ds(0, 31)], id_send)
    def done(i, _):
        z_copy(lax.div(i, NCH), lax.rem(i, NCH)).wait_send()
        return 0
    lax.fori_loop(0, 4 * NCH, done, 0)


def exchange(rows, ids, mom, cen):
    dma = pltpu.SemaphoreType.DMA
    f32 = jnp.float32
    table = jax.ShapeDtypeStruct((ROWS, 512), f32)
    return pl.pallas_call(
        kernel,
        out_shape=(table, jax.ShapeDtypeStruct((1, 128), f32), table, table),
        in_specs=[pl.BlockSpec(memory_space=pltpu.HBM)] * 4,
        out_specs=(pl.BlockSpec(memory_space=pltpu.VMEM),) * 4,
        scratch_shapes=[
            pltpu.VMEM((128, CAP, WIDE), jnp.bfloat16),
            pltpu.VMEM((32, NZ, 1, CAP), jnp.int32),
            pltpu.VMEM((RING, LOW, UNIT * CAP), BF),
            pltpu.VMEM((RING * UNIT, CAP, WIDE), BF),
            pltpu.VMEM((UNIT * CAP, HIGH * WIDE), BF),
            pltpu.VMEM((4, ROWS, WIDE), f32),
            pltpu.VMEM((4, ROWS, WIDE), f32),
            pltpu.VMEM((ROWS, WIDE), f32),
            pltpu.VMEM((NCH, HALF, WIDE), f32),
            pltpu.VMEM((32, 1, 128), f32),
            pltpu.VMEM((NZ, 1, 128), f32),
            dma((5,)), dma((8,)), dma, dma,
            dma((4, NCH)), dma((4, NCH)), dma((NCH,)), dma((NCH,)),
            dma((NCH, 4)), dma((NCH, 4)), dma((NCH, 5)), dma((NCH, 5)),
            dma, dma, dma, dma, dma((2,)),
        ],
        compiler_params=pltpu.CompilerParams(collective_id=0, has_side_effects=True,
                                             vmem_limit_bytes=40 * 2 ** 20),
        name="exchange",
    )(rows, ids, mom, cen)


def update_kernel(sq, g, m, cen, new_c, new_m, held_c, held_m, sent):
    squares = jnp.sum(sq[...], keepdims=True)
    factor = jnp.minimum(1.0, clip_rms * math.sqrt(65536 * 512) / jnp.sqrt(squares + eps_norm))

    def copies(i):
        at = pl.ds(pl.multiple_of(i * TILE, TILE), TILE)
        return (pltpu.make_async_copy(held_m.at[at], new_m.at[at], sent.at[0, i]),
                pltpu.make_async_copy(held_c.at[at], new_c.at[at], sent.at[1, i]))

    def tile(i, _):
        at = pl.ds(pl.multiple_of(i * TILE, TILE), TILE)
        mom = beta_decay * m[at] + factor * g[at]
        held_m[at] = mom
        stepped = cen[at] - learn_rate * mom
        rescale = lax.rsqrt(jnp.mean(stepped * stepped, axis=1, keepdims=True) + eps_row)
        held_c[at] = stepped * rescale
        for copy in copies(i):
            copy.start()
        return 0
    lax.fori_loop(0, ROWS // TILE, tile, 0)

    def drain(i, _):
        for copy in copies(i):
            copy.wait()
        return 0
    lax.fori_loop(0, ROWS // TILE, drain, 0)


def update(sq, g, m, cen):
    shape = jax.ShapeDtypeStruct((ROWS, 512), jnp.float32)
    return pl.pallas_call(
        update_kernel,
        out_shape=(shape, shape),
        in_specs=[pl.BlockSpec(memory_space=pltpu.VMEM)] * 4,
        out_specs=(pl.BlockSpec(memory_space=pltpu.HBM),) * 2,
        scratch_shapes=[
            pltpu.VMEM((ROWS, 512), jnp.float32),
            pltpu.VMEM((ROWS, 512), jnp.float32),
            pltpu.SemaphoreType.DMA((2, ROWS // TILE)),
        ],
        compiler_params=pltpu.CompilerParams(vmem_limit_bytes=24 * 2 ** 20),
        name="update",
    )(sq, g, m, cen)


def on_device(centers, momentum, grad_rows, row_ids):
    g, sq, mom, cen = exchange(
        grad_rows.reshape(32, CAP, 512), row_ids.reshape(NZ, NY, 1, CAP), momentum, centers)
    return update(sq, g, mom, cen)


def solution(mesh):
    placed = (P("cls", None), P("cls", None), P(("dp", "cls"), None), P(("dp", "cls")))
    return jax.shard_map(
        on_device,
        mesh=mesh,
        in_specs=placed,
        out_specs=(P("cls", None), P("cls", None)),
        check_vma=False,
    )
```

```python
import functools, math
import jax
import jax.numpy as jnp
from jax import lax
from jax.experimental import pallas as pl
from jax.experimental.pallas import tpu as pltpu
from jax.sharding import PartitionSpec as P

MESH = pl.DeviceIdType.MESH
BF = jnp.bfloat16
NX, NY, NZ = 4, 4, 8
CAP, WIDE = 128, 128
ROWS = 2048
UNIT = NX * NY
HIGH = 4
LOW = ROWS // HIGH
NCH = 8
CH = ROWS // NCH
HALF = CH // 2
LAG_D, LAG_A, LAG_F, LAG_S = 2, 5, 9, 2
TILE = 128
RING = 4
COUNT = (16, 32, 32, 32, 16)
UNITS = ((0,), (1, 2), (3, 4), (5, 6), (7,))
PIECE = (0, 1, 1, 2, 2, 3, 3, 4)
beta_decay, learn_rate, clip_rms, eps_norm, eps_row = 0.9, 0.5, 1.0, 1e-06, 1e-06


def wrap(a, n):
    return lax.rem(a + n, n)


def kernel(rows, ids, mom, cen, g_out, sq_out, mom_out, cen_out, raw, idr, hot, high, wide, zs, zr, zsw, fp, dsw, sq1, sq2,
           raw_send, raw_recv, id_send, id_recv, z_send, z_recv, d_send, d_recv,
           a_send, a_recv, f_send, f_recv, s1_send, s1_recv, s2_send, s2_recv, keep, t_send, t_recv):
    d, g = lax.axis_index("dp"), lax.axis_index("cls")
    x, c = lax.div(d, 2), lax.rem(d, 2)
    z, y = lax.div(g, NY), lax.rem(g, NY)
    sgn = 1 - 2 * c
    other = 1 - c

    def dev(xx, cc, yy, zz):
        return (xx * 2 + cc, zz * NY + yy)

    bar = pltpu.get_barrier_semaphore()

    def greet_plane(j, _):
        cc, xx, yy = lax.rem(j, 2), lax.div(j, 8), lax.rem(lax.div(j, 2), NY)
        @pl.when(jnp.logical_or(jnp.logical_or(cc != c, xx != x), yy != y))
        def _():
            pl.semaphore_signal(bar, 1, device_id=dev(xx, cc, yy, z), device_id_type=MESH)
        return 0
    lax.fori_loop(0, 32, greet_plane, 0)

    def greet_z(j, _):
        pl.semaphore_signal(bar, 1, device_id=dev(x, c, y, wrap(z + j, NZ)), device_id_type=MESH)
        return 0
    lax.fori_loop(1, NZ, greet_z, 0)
    pl.semaphore_wait(bar, 31 + NZ - 1)

    me32 = c * UNIT + x * NY + y

    def place(t, dx):
        return t * 2 * NX + dx * 2 + c

    def id_round(t, _):
        for dx in range(NX):
            for cc in range(2):
                xx, yy = lax.rem(x + dx, NX), lax.rem(y + dx + t + c, NY)

                def send():
                    pltpu.make_async_remote_copy(
                        ids.at[:, yy], idr.at[place(t, dx)], id_send, id_recv,
                        device_id=dev(xx, cc, yy, z), device_id_type=MESH).start()
                if dx:
                    send()
                else:
                    pl.when(jnp.logical_or(yy != y, cc != c))(send)
        return 0
    lax.fori_loop(0, NY, id_round, 0)
    home = lax.rem(NY - c, NY)
    pltpu.make_async_copy(ids.at[:, y], idr.at[place(home, 0)], id_recv).start()

    def momentum_in():
        pltpu.make_async_copy(mom, mom_out, keep.at[0]).start()
        pltpu.make_async_copy(cen, cen_out, keep.at[1]).start()

    def send_piece(p):
        k = 4 - p
        full = COUNT[p] == 32
        near, away = wrap(z + (sgn if full else 1) * k, NZ), wrap(z - sgn * k, NZ)

        def where_to(t, dx):
            if full:
                unit = UNITS[p][0] + lax.div(t, 2)
                return unit, UNITS[p][0] * UNIT + place(t, dx)
            return UNITS[p][0], UNITS[p][0] * UNIT + t * NX + dx

        def lines(xx, yy, zz):
            return rows.at[zz * NY + yy, :, pl.ds(pl.multiple_of(xx * WIDE, WIDE), WIDE)]

        def remote(t, dx, xx, yy, cc, zz):
            unit, slot = where_to(t, dx)
            pltpu.make_async_remote_copy(lines(xx, yy, zz), raw.at[slot], raw_send.at[p], raw_recv.at[unit],
                                         device_id=dev(xx, cc, yy, z), device_id_type=MESH).start()

        def round_of(t, _):
            for dx in range(NX):
                xx, yy = lax.rem(x + dx, NX), lax.rem(y + dx + t + c, NY)

                def both():
                    remote(t, dx, xx, yy, c, near)
                    if full:
                        remote(t, dx, xx, yy, other, away)
                if dx:
                    both()
                else:
                    pl.when(yy != y)(both)
            return 0
        lax.fori_loop(0, NY, round_of, 0)
        if full:
            remote(home, 0, x, y, other, away)
        unit, slot = where_to(home, 0)
        pltpu.make_async_copy(lines(x, y, near), raw.at[slot], raw_recv.at[unit]).start()

    def all_in(ref, sem):
        pltpu.make_async_copy(ref, ref, sem).wait()

    def unit_in(u):
        all_in(raw.at[pl.ds(u * UNIT, UNIT)], raw_recv.at[u])

    def piece_out(p):
        all_in(raw.at[pl.ds(0, COUNT[p] - 1)], raw_send.at[p])

    def prepare(u):
        p = PIECE[u]
        zz = wrap(z + sgn * (4 - p), NZ)
        base = (zz * NY + y) * ROWS

        def local(b):
            at = 2 * b + c if COUNT[p] == 16 else (u + 1) % 2 * UNIT + b
            return idr[at, zz] - base

        def block(b, _):
            part = jnp.right_shift(local(b), LOW.bit_length() - 1).astype(jnp.float32)
            high[u % RING * UNIT + b] = jnp.broadcast_to(part, (CAP, WIDE)).T.astype(BF)
            return 0
        lax.fori_loop(0, UNIT, block, 0, unroll=4)
        line = lax.broadcasted_iota(jnp.int32, (LOW, 2 * CAP), 0)
        for q in range(UNIT // 2):
            low = jnp.bitwise_and(jnp.concatenate([local(2 * q), local(2 * q + 1)], axis=1), LOW - 1)
            hot[u % RING, :, q * 2 * CAP:(q + 1) * 2 * CAP] = jnp.where(line == low, 1.0, 0.0).astype(BF)

    def compute(u, out, add):
        for b in range(UNIT):
            lines, part = raw[u * UNIT + b], high[u % RING * UNIT + b]
            for h in range(HIGH):
                wide[b * CAP:(b + 1) * CAP, h * WIDE:(h + 1) * WIDE] = jnp.where(
                    part == jnp.asarray(h, BF), lines, jnp.zeros_like(lines))
        for n in range(HIGH // 2):
            v = jnp.dot(hot[u % RING], wide[:, 2 * n * WIDE:2 * (n + 1) * WIDE], preferred_element_type=jnp.float32)
            for q in range(2):
                at = pl.ds((2 * n + q) * LOW, LOW)
                now = v[:, q * WIDE:(q + 1) * WIDE]
                out[at, :] = out[at, :] + now if add else now

    up = wrap(z + sgn, NZ)

    def rows_at(r):
        return pl.ds(pl.multiple_of(r * CH, CH), CH)

    def z_copy(p, r):
        return pltpu.make_async_remote_copy(
            zs.at[p, rows_at(r)], zr.at[p, rows_at(r)], z_send.at[p, r], z_recv.at[p, r],
            device_id=dev(x, c, y, up), device_id_type=MESH)

    def trade():
        return pltpu.make_async_remote_copy(
            zs.at[0, pl.ds(pl.multiple_of(other * (ROWS // 2), ROWS // 2), ROWS // 2)], zsw,
            t_send, t_recv, device_id=dev(x, other, y, z), device_id_type=MESH)

    for p in range(2):
        send_piece(p)
    momentum_in()
    all_in(idr, id_recv)
    for u in range(3):
        prepare(u)
    for p in range(4):
        if p + 2 < 5:
            send_piece(p + 2)
        for u in UNITS[p]:
            unit_in(u)
            compute(u, zs.at[p], u != UNITS[p][0])

        def fresh(i, _):
            z_copy(p, other * (NCH // 2) + i).start()
            return 0

        def shared(i, _):
            r = c * (NCH // 2) + i
            if p:
                z_copy(p - 1, r).wait_recv()
                zs[p, rows_at(r)] = zs[p, rows_at(r)] + zr[p - 1, rows_at(r)]
            else:
                zs[p, rows_at(r)] = zs[p, rows_at(r)] + zsw[rows_at(i)]
            z_copy(p, r).start()
            return 0

        def chunk(r, _):
            z_copy(p - 1, r).wait_recv()
            zs[p, rows_at(r)] = zs[p, rows_at(r)] + zr[p - 1, rows_at(r)]
            z_copy(p, r).start()
            return 0

        if p == 0:
            trade().start()
            trade().wait_recv()
        if p == 1:
            lax.fori_loop(0, NCH // 2, fresh, 0)
        if p < 2:
            lax.fori_loop(0, NCH // 2, shared, 0)
        else:
            lax.fori_loop(0, NCH, chunk, 0)
        for u in UNITS[p]:
            if u + 3 < 8:
                prepare(u + 3)
    unit_in(7)

    mine_x = pl.ds(pl.multiple_of(x * WIDE, WIDE), WIDE)
    compute(7, fp, False)

    def d_copy(r):
        return pltpu.make_async_remote_copy(
            fp.at[pl.ds(lines_of(r, other), HALF)], dsw.at[r], d_send.at[r], d_recv.at[r],
            device_id=dev(x, other, y, z), device_id_type=MESH)

    def lines_of(r, cc):
        return pl.multiple_of(r * CH + cc * HALF, HALF)

    def a_copy(r, way, xx_slab, part, slot, step):
        to_x = wrap(x + 1 - 2 * way, NX)
        size = HALF // 2 if step else HALF
        at = lines_of(r, c) + (part * size if step else 0)
        ref = g_out.at[pl.ds(pl.multiple_of(at, size), size), pl.ds(pl.multiple_of(xx_slab * WIDE, WIDE), WIDE)]
        return pltpu.make_async_remote_copy(
            ref, ref, a_send.at[r, slot], a_recv.at[r, slot],
            device_id=dev(to_x, c, y, z), device_id_type=MESH)

    def f_copy(r, cc, slab, part, slot):
        size = HALF if part is None else HALF // 2
        at = lines_of(r, cc) + (0 if part is None else part * size)
        ref = g_out.at[pl.ds(pl.multiple_of(at, size), size), pl.ds(pl.multiple_of(slab * WIDE, WIDE), WIDE)]
        return pltpu.make_async_remote_copy(
            ref, ref, f_send.at[r, slot], f_recv.at[r, slot],
            device_id=dev(x, other, y, z), device_id_type=MESH)

    right, left, far = wrap(x + 1, NX), wrap(x - 1, NX), wrap(x + 2, NX)
    total = jnp.zeros((8, 128), jnp.float32)
    for t in range(NCH + LAG_F):
        if t < NCH:
            r = t
            z_copy(3, r).wait_recv()
            fp[rows_at(r)] = fp[rows_at(r)] + zr[3, rows_at(r)]
            d_copy(r).start()
        if 0 <= t - LAG_D < NCH:
            r = t - LAG_D
            d_copy(r).wait_recv()
            own = fp[pl.ds(lines_of(r, c), HALF)] + dsw[r]
            g_out[pl.ds(lines_of(r, c), HALF), mine_x] = own
            a_copy(r, 0, x, 0, 0, 0).start()
            a_copy(r, 1, x, 0, 1, 0).start()
            f_copy(r, c, x, None, 0).start()
            total = total + jnp.sum((own * own).reshape(HALF // 8, 8, 128), axis=0)
        if t == NCH - 1 + LAG_D:
            sq2[z] = jnp.sum(total, axis=0, keepdims=True)

            def sq_up(j, _):
                pltpu.make_async_remote_copy(
                    sq2.at[z], sq2.at[z], s2_send, s2_recv,
                    device_id=dev(x, c, y, wrap(z + j, NZ)), device_id_type=MESH).start()
                return 0
            lax.fori_loop(1, NZ, sq_up, 0)
        if 0 <= t - LAG_A < NCH:
            r = t - LAG_A
            a_copy(r, 0, left, 0, 0, 0).wait_recv()
            f_copy(r, c, left, None, 1).start()
            a_copy(r, 0, left, 0, 2, 1).start()
            a_copy(r, 1, right, 0, 1, 0).wait_recv()
            f_copy(r, c, right, None, 2).start()
            a_copy(r, 1, right, 1, 3, 1).start()
        if 0 <= t - LAG_F < NCH:
            r = t - LAG_F
            a_copy(r, 0, far, 0, 2, 1).wait_recv()
            f_copy(r, c, far, 0, 3).start()
            a_copy(r, 1, far, 1, 3, 1).wait_recv()
            f_copy(r, c, far, 1, 4).start()
        if t == NCH - 1 + LAG_D + LAG_S:
            all_in(sq2.at[pl.ds(0, NZ - 1)], s2_recv)
            sq1[me32] = jnp.sum(sq2[...], axis=0)

            def sq_to(j, _):
                cc, xx, yy = lax.rem(j, 2), lax.div(j, 8), lax.rem(lax.div(j, 2), NY)
                @pl.when(jnp.logical_or(jnp.logical_or(cc != c, xx != x), yy != y))
                def _():
                    pltpu.make_async_remote_copy(
                        sq1.at[me32], sq1.at[me32], s1_send, s1_recv,
                        device_id=dev(xx, cc, yy, z), device_id_type=MESH).start()
                return 0
            lax.fori_loop(0, 32, sq_to, 0)
    for r in range(NCH):
        f_copy(r, other, x, None, 0).wait_recv()
        f_copy(r, other, left, None, 1).wait_recv()
        f_copy(r, other, right, None, 2).wait_recv()
        f_copy(r, other, far, 0, 3).wait_recv()
        f_copy(r, other, far, 1, 4).wait_recv()
    all_in(sq1.at[pl.ds(0, 31)], s1_recv)
    sq_out[...] = jnp.sum(sq1[...], axis=0)
    for r in range(NCH):
        d_copy(r).wait_send()
        for slot, step in ((0, 0), (1, 0), (2, 1), (3, 1)):
            a_copy(r, 0, x, 0, slot, step).wait_send()
        for slot, part in ((0, None), (1, None), (2, None), (3, 0), (4, 1)):
            f_copy(r, c, x, part, slot).wait_send()
    all_in(sq1.at[pl.ds(0, 31)], s1_send)
    all_in(sq2.at[pl.ds(0, NZ - 1)], s2_send)
    pltpu.make_async_copy(mom, mom_out, keep.at[0]).wait()
    pltpu.make_async_copy(cen, cen_out, keep.at[1]).wait()
    for p in range(5):
        piece_out(p)
    all_in(idr.at[pl.ds(0, 31)], id_send)
    def done(i, _):
        z_copy(lax.div(i, NCH), lax.rem(i, NCH)).wait_send()
        return 0
    lax.fori_loop(NCH, 4 * NCH, done, 0)

    def done_first(i, _):
        z_copy(0, c * (NCH // 2) + i).wait_send()
        return 0
    lax.fori_loop(0, NCH // 2, done_first, 0)
    trade().wait_send()


def exchange(rows, ids, mom, cen):
    dma = pltpu.SemaphoreType.DMA
    f32 = jnp.float32
    table = jax.ShapeDtypeStruct((ROWS, 512), f32)
    return pl.pallas_call(
        kernel,
        out_shape=(table, jax.ShapeDtypeStruct((1, 128), f32), table, table),
        in_specs=[pl.BlockSpec(memory_space=pltpu.HBM)] * 4,
        out_specs=(pl.BlockSpec(memory_space=pltpu.VMEM),) * 4,
        scratch_shapes=[
            pltpu.VMEM((128, CAP, WIDE), jnp.bfloat16),
            pltpu.VMEM((32, NZ, 1, CAP), jnp.int32),
            pltpu.VMEM((RING, LOW, UNIT * CAP), BF),
            pltpu.VMEM((RING * UNIT, CAP, WIDE), BF),
            pltpu.VMEM((UNIT * CAP, HIGH * WIDE), BF),
            pltpu.VMEM((4, ROWS, WIDE), f32),
            pltpu.VMEM((4, ROWS, WIDE), f32),
            pltpu.VMEM((ROWS // 2, WIDE), f32),
            pltpu.VMEM((ROWS, WIDE), f32),
            pltpu.VMEM((NCH, HALF, WIDE), f32),
            pltpu.VMEM((32, 1, 128), f32),
            pltpu.VMEM((NZ, 1, 128), f32),
            dma((5,)), dma((8,)), dma, dma,
            dma((4, NCH)), dma((4, NCH)), dma((NCH,)), dma((NCH,)),
            dma((NCH, 4)), dma((NCH, 4)), dma((NCH, 5)), dma((NCH, 5)),
            dma, dma, dma, dma, dma((2,)), dma, dma,
        ],
        compiler_params=pltpu.CompilerParams(collective_id=0, has_side_effects=True,
                                             vmem_limit_bytes=40 * 2 ** 20),
        name="exchange",
    )(rows, ids, mom, cen)


def update_kernel(sq, g, m, cen, new_c, new_m, held_c, held_m, sent):
    squares = jnp.sum(sq[...], keepdims=True)
    factor = jnp.minimum(1.0, clip_rms * math.sqrt(65536 * 512) / jnp.sqrt(squares + eps_norm))

    def copies(i):
        at = pl.ds(pl.multiple_of(i * TILE, TILE), TILE)
        return (pltpu.make_async_copy(held_m.at[at], new_m.at[at], sent.at[0, i]),
                pltpu.make_async_copy(held_c.at[at], new_c.at[at], sent.at[1, i]))

    def tile(i, _):
        at = pl.ds(pl.multiple_of(i * TILE, TILE), TILE)
        mom = beta_decay * m[at] + factor * g[at]
        held_m[at] = mom
        stepped = cen[at] - learn_rate * mom
        rescale = lax.rsqrt(jnp.mean(stepped * stepped, axis=1, keepdims=True) + eps_row)
        held_c[at] = stepped * rescale
        for copy in copies(i):
            copy.start()
        return 0
    lax.fori_loop(0, ROWS // TILE, tile, 0)

    def drain(i, _):
        for copy in copies(i):
            copy.wait()
        return 0
    lax.fori_loop(0, ROWS // TILE, drain, 0)


def update(sq, g, m, cen):
    shape = jax.ShapeDtypeStruct((ROWS, 512), jnp.float32)
    return pl.pallas_call(
        update_kernel,
        out_shape=(shape, shape),
        in_specs=[pl.BlockSpec(memory_space=pltpu.VMEM)] * 4,
        out_specs=(pl.BlockSpec(memory_space=pltpu.HBM),) * 2,
        scratch_shapes=[
            pltpu.VMEM((ROWS, 512), jnp.float32),
            pltpu.VMEM((ROWS, 512), jnp.float32),
            pltpu.SemaphoreType.DMA((2, ROWS // TILE)),
        ],
        compiler_params=pltpu.CompilerParams(vmem_limit_bytes=24 * 2 ** 20),
        name="update",
    )(sq, g, m, cen)


def on_device(centers, momentum, grad_rows, row_ids):
    g, sq, mom, cen = exchange(
        grad_rows.reshape(32, CAP, 512), row_ids.reshape(NZ, NY, 1, CAP), momentum, centers)
    return update(sq, g, mom, cen)


def solution(mesh):
    placed = (P("cls", None), P("cls", None), P(("dp", "cls"), None), P(("dp", "cls")))
    return jax.shard_map(
        on_device,
        mesh=mesh,
        in_specs=placed,
        out_specs=(P("cls", None), P("cls", None)),
        check_vma=False,
    )
```

```python
import functools, math
import jax
import jax.numpy as jnp
from jax import lax
from jax.experimental import pallas as pl
from jax.experimental.pallas import tpu as pltpu
from jax.sharding import PartitionSpec as P

MESH = pl.DeviceIdType.MESH
BF = jnp.bfloat16
NX, NY, NZ = 4, 4, 8
CAP, WIDE = 128, 128
ROWS = 2048
UNIT = NX * NY
HIGH = 4
LOW = ROWS // HIGH
NCH = 8
CH = ROWS // NCH
HALF = CH // 2
LAG_D, LAG_A, LAG_F, LAG_S = 2, 6, 11, 2
TILE = 128
RING = 4
COUNT = (16, 32, 32, 32, 16)
UNITS = ((0,), (1, 2), (3, 4), (5, 6), (7,))
PIECE = (0, 1, 1, 2, 2, 3, 3, 4)
beta_decay, learn_rate, clip_rms, eps_norm, eps_row = 0.9, 0.5, 1.0, 1e-06, 1e-06


def wrap(a, n):
    return lax.rem(a + n, n)


def kernel(rows, ids, mom, cen, g_out, sq_out, mom_out, cen_out, raw, idr, hot, high, wide, zs, zr, zsw, fp, dsw, sq1, sq2,
           raw_send, raw_recv, id_send, id_recv, z_send, z_recv, d_send, d_recv,
           a_send, a_recv, f_send, f_recv, s1_send, s1_recv, s2_send, s2_recv, keep, t_send, t_recv):
    d, g = lax.axis_index("dp"), lax.axis_index("cls")
    x, c = lax.div(d, 2), lax.rem(d, 2)
    z, y = lax.div(g, NY), lax.rem(g, NY)
    sgn = 1 - 2 * c
    other = 1 - c

    def dev(xx, cc, yy, zz):
        return (xx * 2 + cc, zz * NY + yy)

    bar = pltpu.get_barrier_semaphore()

    def greet_plane(j, _):
        cc, xx, yy = lax.rem(j, 2), lax.div(j, 8), lax.rem(lax.div(j, 2), NY)
        @pl.when(jnp.logical_or(jnp.logical_or(cc != c, xx != x), yy != y))
        def _():
            pl.semaphore_signal(bar, 1, device_id=dev(xx, cc, yy, z), device_id_type=MESH)
        return 0
    lax.fori_loop(0, 32, greet_plane, 0)

    def greet_z(j, _):
        pl.semaphore_signal(bar, 1, device_id=dev(x, c, y, wrap(z + j, NZ)), device_id_type=MESH)
        return 0
    lax.fori_loop(1, NZ, greet_z, 0)
    pl.semaphore_wait(bar, 31 + NZ - 1)

    me32 = c * UNIT + x * NY + y

    def place(t, dx):
        return t * 2 * NX + dx * 2 + c

    def id_round(t, _):
        for dx in range(NX):
            for cc in range(2):
                xx, yy = lax.rem(x + dx, NX), lax.rem(y + dx + t + c, NY)

                def send():
                    pltpu.make_async_remote_copy(
                        ids.at[:, yy], idr.at[place(t, dx)], id_send, id_recv,
                        device_id=dev(xx, cc, yy, z), device_id_type=MESH).start()
                if dx:
                    send()
                else:
                    pl.when(jnp.logical_or(yy != y, cc != c))(send)
        return 0
    lax.fori_loop(0, NY, id_round, 0)
    home = lax.rem(NY - c, NY)
    pltpu.make_async_copy(ids.at[:, y], idr.at[place(home, 0)], id_recv).start()

    def momentum_in():
        pltpu.make_async_copy(mom, mom_out, keep.at[0]).start()
        pltpu.make_async_copy(cen, cen_out, keep.at[1]).start()

    def send_piece(p):
        k = 4 - p
        full = COUNT[p] == 32
        near, away = wrap(z + (sgn if full else 1) * k, NZ), wrap(z - sgn * k, NZ)

        def where_to(t, dx):
            if full:
                unit = UNITS[p][0] + lax.div(t, 2)
                return unit, UNITS[p][0] * UNIT + place(t, dx)
            return UNITS[p][0], UNITS[p][0] * UNIT + t * NX + dx

        def lines(xx, yy, zz):
            return rows.at[zz * NY + yy, :, pl.ds(pl.multiple_of(xx * WIDE, WIDE), WIDE)]

        def remote(t, dx, xx, yy, cc, zz):
            unit, slot = where_to(t, dx)
            pltpu.make_async_remote_copy(lines(xx, yy, zz), raw.at[slot], raw_send.at[p], raw_recv.at[unit],
                                         device_id=dev(xx, cc, yy, z), device_id_type=MESH).start()

        def round_of(t, _):
            for dx in range(NX):
                xx, yy = lax.rem(x + dx, NX), lax.rem(y + dx + t + c, NY)

                def both():
                    remote(t, dx, xx, yy, c, near)
                    if full:
                        remote(t, dx, xx, yy, other, away)
                if dx:
                    both()
                else:
                    pl.when(yy != y)(both)
            return 0
        lax.fori_loop(0, NY, round_of, 0)
        if full:
            remote(home, 0, x, y, other, away)
        unit, slot = where_to(home, 0)
        pltpu.make_async_copy(lines(x, y, near), raw.at[slot], raw_recv.at[unit]).start()

    def all_in(ref, sem):
        pltpu.make_async_copy(ref, ref, sem).wait()

    def unit_in(u):
        all_in(raw.at[pl.ds(u * UNIT, UNIT)], raw_recv.at[u])

    def piece_out(p):
        all_in(raw.at[pl.ds(0, COUNT[p] - 1)], raw_send.at[p])

    def prepare(u):
        p = PIECE[u]
        zz = wrap(z + sgn * (4 - p), NZ)
        base = (zz * NY + y) * ROWS

        def local(b):
            at = 2 * b + c if COUNT[p] == 16 else (u + 1) % 2 * UNIT + b
            return idr[at, zz] - base

        def block(b, _):
            part = jnp.right_shift(local(b), LOW.bit_length() - 1).astype(jnp.float32)
            high[u % RING * UNIT + b] = jnp.broadcast_to(part, (CAP, WIDE)).T.astype(BF)
            return 0
        lax.fori_loop(0, UNIT, block, 0, unroll=4)
        line = lax.broadcasted_iota(jnp.int32, (LOW, 2 * CAP), 0)
        for q in range(UNIT // 2):
            low = jnp.bitwise_and(jnp.concatenate([local(2 * q), local(2 * q + 1)], axis=1), LOW - 1)
            hot[u % RING, :, q * 2 * CAP:(q + 1) * 2 * CAP] = jnp.where(line == low, 1.0, 0.0).astype(BF)

    def compute(u, out, add):
        for b in range(UNIT):
            lines, part = raw[u * UNIT + b], high[u % RING * UNIT + b]
            for h in range(HIGH):
                wide[b * CAP:(b + 1) * CAP, h * WIDE:(h + 1) * WIDE] = jnp.where(
                    part == jnp.asarray(h, BF), lines, jnp.zeros_like(lines))
        for n in range(HIGH // 2):
            v = jnp.dot(hot[u % RING], wide[:, 2 * n * WIDE:2 * (n + 1) * WIDE], preferred_element_type=jnp.float32)
            for q in range(2):
                at = pl.ds((2 * n + q) * LOW, LOW)
                now = v[:, q * WIDE:(q + 1) * WIDE]
                out[at, :] = out[at, :] + now if add else now

    up = wrap(z + sgn, NZ)

    def rows_at(r):
        return pl.ds(pl.multiple_of(r * CH, CH), CH)

    def z_copy(p, r):
        return pltpu.make_async_remote_copy(
            zs.at[p, rows_at(r)], zr.at[p, rows_at(r)], z_send.at[p, r], z_recv.at[p, r],
            device_id=dev(x, c, y, up), device_id_type=MESH)

    def trade():
        return pltpu.make_async_remote_copy(
            zs.at[0, pl.ds(pl.multiple_of(other * (ROWS // 2), ROWS // 2), ROWS // 2)], zsw,
            t_send, t_recv, device_id=dev(x, other, y, z), device_id_type=MESH)

    for p in range(2):
        send_piece(p)
    momentum_in()
    all_in(idr, id_recv)
    for u in range(3):
        prepare(u)
    for p in range(4):
        if p + 2 < 5:
            send_piece(p + 2)
        for u in UNITS[p]:
            unit_in(u)
            compute(u, zs.at[p], u != UNITS[p][0])

        def fresh(i, _):
            z_copy(p, other * (NCH // 2) + i).start()
            return 0

        def shared(i, _):
            r = c * (NCH // 2) + i
            if p:
                z_copy(p - 1, r).wait_recv()
                zs[p, rows_at(r)] = zs[p, rows_at(r)] + zr[p - 1, rows_at(r)]
            else:
                zs[p, rows_at(r)] = zs[p, rows_at(r)] + zsw[rows_at(i)]
            z_copy(p, r).start()
            return 0

        def chunk(r, _):
            z_copy(p - 1, r).wait_recv()
            zs[p, rows_at(r)] = zs[p, rows_at(r)] + zr[p - 1, rows_at(r)]
            z_copy(p, r).start()
            return 0

        if p == 0:
            trade().start()
            trade().wait_recv()
        if p == 1:
            lax.fori_loop(0, NCH // 2, fresh, 0)
        if p < 2:
            lax.fori_loop(0, NCH // 2, shared, 0)
        else:
            lax.fori_loop(0, NCH, chunk, 0)
        for u in UNITS[p]:
            if u + 3 < 8:
                prepare(u + 3)
    unit_in(7)

    mine_x = pl.ds(pl.multiple_of(x * WIDE, WIDE), WIDE)
    compute(7, fp, False)

    def d_copy(r):
        return pltpu.make_async_remote_copy(
            fp.at[pl.ds(lines_of(r, other), HALF)], dsw.at[r], d_send.at[r], d_recv.at[r],
            device_id=dev(x, other, y, z), device_id_type=MESH)

    def lines_of(r, cc):
        return pl.multiple_of(r * CH + cc * HALF, HALF)

    def a_copy(r, way, xx_slab, part, slot, step):
        to_x = wrap(x + 1 - 2 * way, NX)
        size = HALF // 2 if step else HALF
        at = lines_of(r, c) + (part * size if step else 0)
        ref = g_out.at[pl.ds(pl.multiple_of(at, size), size), pl.ds(pl.multiple_of(xx_slab * WIDE, WIDE), WIDE)]
        return pltpu.make_async_remote_copy(
            ref, ref, a_send.at[r, slot], a_recv.at[r, slot],
            device_id=dev(to_x, c, y, z), device_id_type=MESH)

    def f_copy(r, cc, slab, part, slot):
        size = HALF if part is None else HALF // 2
        at = lines_of(r, cc) + (0 if part is None else part * size)
        ref = g_out.at[pl.ds(pl.multiple_of(at, size), size), pl.ds(pl.multiple_of(slab * WIDE, WIDE), WIDE)]
        return pltpu.make_async_remote_copy(
            ref, ref, f_send.at[r, slot], f_recv.at[r, slot],
            device_id=dev(x, other, y, z), device_id_type=MESH)

    right, left, far = wrap(x + 1, NX), wrap(x - 1, NX), wrap(x + 2, NX)
    total = jnp.zeros((8, 128), jnp.float32)
    for t in range(NCH + LAG_F):
        if t < NCH:
            r = t
            z_copy(3, r).wait_recv()
            fp[rows_at(r)] = fp[rows_at(r)] + zr[3, rows_at(r)]
            d_copy(r).start()
        if 0 <= t - LAG_D < NCH:
            r = t - LAG_D
            d_copy(r).wait_recv()
            own = fp[pl.ds(lines_of(r, c), HALF)] + dsw[r]
            g_out[pl.ds(lines_of(r, c), HALF), mine_x] = own
            a_copy(r, 0, x, 0, 0, 0).start()
            a_copy(r, 1, x, 0, 1, 0).start()
            f_copy(r, c, x, None, 0).start()
            total = total + jnp.sum((own * own).reshape(HALF // 8, 8, 128), axis=0)
        if t == NCH - 1 + LAG_D:
            sq2[z] = jnp.sum(total, axis=0, keepdims=True)

            def sq_up(j, _):
                pltpu.make_async_remote_copy(
                    sq2.at[z], sq2.at[z], s2_send, s2_recv,
                    device_id=dev(x, c, y, wrap(z + j, NZ)), device_id_type=MESH).start()
                return 0
            lax.fori_loop(1, NZ, sq_up, 0)
        if 0 <= t - LAG_A < NCH:
            r = t - LAG_A
            a_copy(r, 0, left, 0, 0, 0).wait_recv()
            f_copy(r, c, left, None, 1).start()
            a_copy(r, 0, left, 0, 2, 1).start()
            a_copy(r, 1, right, 0, 1, 0).wait_recv()
            f_copy(r, c, right, None, 2).start()
            a_copy(r, 1, right, 1, 3, 1).start()
        if 0 <= t - LAG_F < NCH:
            r = t - LAG_F
            a_copy(r, 0, far, 0, 2, 1).wait_recv()
            f_copy(r, c, far, 0, 3).start()
            a_copy(r, 1, far, 1, 3, 1).wait_recv()
            f_copy(r, c, far, 1, 4).start()
        if t == NCH - 1 + LAG_D + LAG_S:
            all_in(sq2.at[pl.ds(0, NZ - 1)], s2_recv)
            sq1[me32] = jnp.sum(sq2[...], axis=0)

            def sq_to(j, _):
                cc, xx, yy = lax.rem(j, 2), lax.div(j, 8), lax.rem(lax.div(j, 2), NY)
                @pl.when(jnp.logical_or(jnp.logical_or(cc != c, xx != x), yy != y))
                def _():
                    pltpu.make_async_remote_copy(
                        sq1.at[me32], sq1.at[me32], s1_send, s1_recv,
                        device_id=dev(xx, cc, yy, z), device_id_type=MESH).start()
                return 0
            lax.fori_loop(0, 32, sq_to, 0)
    for r in range(NCH):
        f_copy(r, other, x, None, 0).wait_recv()
        f_copy(r, other, left, None, 1).wait_recv()
        f_copy(r, other, right, None, 2).wait_recv()
        f_copy(r, other, far, 0, 3).wait_recv()
        f_copy(r, other, far, 1, 4).wait_recv()
    all_in(sq1.at[pl.ds(0, 31)], s1_recv)
    sq_out[...] = jnp.sum(sq1[...], axis=0)
    for r in range(NCH):
        d_copy(r).wait_send()
        for slot, step in ((0, 0), (1, 0), (2, 1), (3, 1)):
            a_copy(r, 0, x, 0, slot, step).wait_send()
        for slot, part in ((0, None), (1, None), (2, None), (3, 0), (4, 1)):
            f_copy(r, c, x, part, slot).wait_send()
    all_in(sq1.at[pl.ds(0, 31)], s1_send)
    all_in(sq2.at[pl.ds(0, NZ - 1)], s2_send)
    pltpu.make_async_copy(mom, mom_out, keep.at[0]).wait()
    pltpu.make_async_copy(cen, cen_out, keep.at[1]).wait()
    for p in range(5):
        piece_out(p)
    all_in(idr.at[pl.ds(0, 31)], id_send)
    def done(i, _):
        z_copy(lax.div(i, NCH), lax.rem(i, NCH)).wait_send()
        return 0
    lax.fori_loop(NCH, 4 * NCH, done, 0)

    def done_first(i, _):
        z_copy(0, c * (NCH // 2) + i).wait_send()
        return 0
    lax.fori_loop(0, NCH // 2, done_first, 0)
    trade().wait_send()


def exchange(rows, ids, mom, cen):
    dma = pltpu.SemaphoreType.DMA
    f32 = jnp.float32
    table = jax.ShapeDtypeStruct((ROWS, 512), f32)
    return pl.pallas_call(
        kernel,
        out_shape=(table, jax.ShapeDtypeStruct((1, 128), f32), table, table),
        in_specs=[pl.BlockSpec(memory_space=pltpu.HBM)] * 4,
        out_specs=(pl.BlockSpec(memory_space=pltpu.VMEM),) * 4,
        scratch_shapes=[
            pltpu.VMEM((128, CAP, WIDE), jnp.bfloat16),
            pltpu.VMEM((32, NZ, 1, CAP), jnp.int32),
            pltpu.VMEM((RING, LOW, UNIT * CAP), BF),
            pltpu.VMEM((RING * UNIT, CAP, WIDE), BF),
            pltpu.VMEM((UNIT * CAP, HIGH * WIDE), BF),
            pltpu.VMEM((4, ROWS, WIDE), f32),
            pltpu.VMEM((4, ROWS, WIDE), f32),
            pltpu.VMEM((ROWS // 2, WIDE), f32),
            pltpu.VMEM((ROWS, WIDE), f32),
            pltpu.VMEM((NCH, HALF, WIDE), f32),
            pltpu.VMEM((32, 1, 128), f32),
            pltpu.VMEM((NZ, 1, 128), f32),
            dma((5,)), dma((8,)), dma, dma,
            dma((4, NCH)), dma((4, NCH)), dma((NCH,)), dma((NCH,)),
            dma((NCH, 4)), dma((NCH, 4)), dma((NCH, 5)), dma((NCH, 5)),
            dma, dma, dma, dma, dma((2,)), dma, dma,
        ],
        compiler_params=pltpu.CompilerParams(collective_id=0, has_side_effects=True,
                                             vmem_limit_bytes=40 * 2 ** 20),
        name="exchange",
    )(rows, ids, mom, cen)


def update_kernel(sq, g, m, cen, new_c, new_m, held_c, held_m, sent):
    squares = jnp.sum(sq[...], keepdims=True)
    factor = jnp.minimum(1.0, clip_rms * math.sqrt(65536 * 512) / jnp.sqrt(squares + eps_norm))

    def copies(i):
        at = pl.ds(pl.multiple_of(i * TILE, TILE), TILE)
        return (pltpu.make_async_copy(held_m.at[at], new_m.at[at], sent.at[0, i]),
                pltpu.make_async_copy(held_c.at[at], new_c.at[at], sent.at[1, i]))

    def tile(i, _):
        at = pl.ds(pl.multiple_of(i * TILE, TILE), TILE)
        mom = beta_decay * m[at] + factor * g[at]
        held_m[at] = mom
        stepped = cen[at] - learn_rate * mom
        rescale = lax.rsqrt(jnp.mean(stepped * stepped, axis=1, keepdims=True) + eps_row)
        held_c[at] = stepped * rescale
        for copy in copies(i):
            copy.start()
        return 0
    lax.fori_loop(0, ROWS // TILE, tile, 0)

    def drain(i, _):
        for copy in copies(i):
            copy.wait()
        return 0
    lax.fori_loop(0, ROWS // TILE, drain, 0)


def update(sq, g, m, cen):
    shape = jax.ShapeDtypeStruct((ROWS, 512), jnp.float32)
    return pl.pallas_call(
        update_kernel,
        out_shape=(shape, shape),
        in_specs=[pl.BlockSpec(memory_space=pltpu.VMEM)] * 4,
        out_specs=(pl.BlockSpec(memory_space=pltpu.HBM),) * 2,
        scratch_shapes=[
            pltpu.VMEM((ROWS, 512), jnp.float32),
            pltpu.VMEM((ROWS, 512), jnp.float32),
            pltpu.SemaphoreType.DMA((2, ROWS // TILE)),
        ],
        compiler_params=pltpu.CompilerParams(vmem_limit_bytes=24 * 2 ** 20),
        name="update",
    )(sq, g, m, cen)


def on_device(centers, momentum, grad_rows, row_ids):
    g, sq, mom, cen = exchange(
        grad_rows.reshape(32, CAP, 512), row_ids.reshape(NZ, NY, 1, CAP), momentum, centers)
    return update(sq, g, mom, cen)


def solution(mesh):
    placed = (P("cls", None), P("cls", None), P(("dp", "cls"), None), P(("dp", "cls")))
    return jax.shard_map(
        on_device,
        mesh=mesh,
        in_specs=placed,
        out_specs=(P("cls", None), P("cls", None)),
        check_vma=False,
    )
```
